32 devices in a mesh: half: 2 (over core), grp: 16 (over z, y, x).
Axes of the slice: x: 2, y: 2, z: 4, core: 2. Of those that a mesh axis runs over, the one named last changes fastest.
Arguments:
- weights: float32 [2, 16, 2, 8192, 128], P('half', 'grp'), may hold values from -4 to 4
- accum: float32 [2, 16, 2, 8192], P('half', 'grp'), may hold values from 0.01 to 1
- grads: float32 [32, 32, 16, 128], P(('half', 'grp')), may hold values from -6 to 6
- row_ids: int32 [32, 32, 16], P(('half', 'grp')), may hold values from 0 to 16383
- counts: int32 [32, 32], P(('half', 'grp')), may hold values from 1 to 16, as said below
Outputs:
- new_weights: float32 [2, 16, 2, 8192, 128], P('half', 'grp')
- new_accum: float32 [2, 16, 2, 8192], P('half', 'grp')
The draws below stay inside these ranges and needn't reach their ends.
Inputs may be any that keep to these rules, and one draw needn't show every extreme that they name: `counts`: A few owners, the same for all senders, receive 16 live rows from every sender; no two of them share a shard index g (owners g and 16 + g). The owner that shares its shard index with such an owner receives 16 // 2 live rows from every sender; each other count lies from 1 to 8. So the two owners of one shard index receive at most 24 live rows from one sender together, and some pair receives exactly that.
All inputs are finite; a program needn't handle non-finite values.
Results may differ from the reference program's by a relative error of at most 0.00002.
Values sent between devices are 32-bit elements; how exact they have to be, the bound alone decides.
A program may use at most 128 MiB of HBM per device.

```python
import math
import jax
import jax.numpy as jnp
import numpy as np
from jax import lax

E = 128
HR = 8192
SLOTS = 16
N_GRP = 16
DEVICES = 32


heavy_owners = 8


def draw_counts(key, part):
    first, second, third = jax.random.split(jax.random.fold_in(key, 11), 3)
    groups = DEVICES // 2
    base = jax.random.randint(first, (DEVICES, DEVICES), 1, SLOTS // 2 + 1)
    ranked = jax.random.permutation(second, groups)
    heavy_group = ranked < heavy_owners
    heavy_bit = jax.random.randint(third, (groups,), 0, 2)
    owner = jnp.arange(DEVICES, dtype=jnp.int32)
    owner_half = owner // groups
    owner_group = owner % groups
    in_heavy = heavy_group[owner_group]
    heavy = in_heavy & (owner_half == heavy_bit[owner_group])
    partner = in_heavy & jnp.logical_not(heavy)
    result = jnp.where(heavy[None, :], SLOTS, jnp.where(partner[None, :], SLOTS // 2, base))
    return result.astype(jnp.int32)


def place_ends(values, stream_key, low, largest):
    longest = values.shape.index(max(values.shape))
    spots = []
    for shift in (0, 1):
        where = [jax.random.randint(jax.random.fold_in(stream_key, axis), (), 0, length) for axis, length in enumerate(values.shape)]
        where[longest] = (where[longest] + shift) % values.shape[longest]
        spots.append(tuple(where))
    return values.at[spots[0]].set(low).at[spots[1]].set(largest)


def raised(values, key, source, target, blocks, factor):
    owner, partner = [(jnp.arange(values.shape[position]) // (values.shape[position] // blocks)).reshape([-1 if axis == position else 1 for axis in range(values.ndim)]) for position in (source, target)]
    chosen = jax.random.permutation(key, blocks)[partner]
    strong = (owner == chosen) | (owner == (partner + blocks // 2) % blocks)
    return jnp.where(strong, factor * values, values)


def block_scale(rng, dims, pieces, low, high):
    def one(axis_at, parts):
        steps = jax.random.uniform(jax.random.fold_in(jax.random.fold_in(rng, 6), axis_at), (parts,), jnp.float32, low / len(pieces), high / len(pieces))
        return jnp.repeat(jnp.exp(steps), dims[axis_at] // parts).reshape((-1,) + (1,) * (len(dims) - axis_at - 1))

    factor_of = one(*pieces[0])
    for cut in pieces[1:]:
        factor_of = factor_of * one(*cut)
    return factor_of


def rank_bounds(number_of, lean):
    loads = [(1 << 20) // math.isqrt(rank ** lean) + 1 for rank in range(1, number_of + 1)]
    spread = 1 + sum(loads) // (1 << 30)
    return np.cumsum(np.array([max(1, weight // spread) for weight in loads]))


def ranked_ids(stream_key, dims, number_of, slope):
    grid = rank_bounds(number_of, slope)
    pick = jax.random.randint(jax.random.fold_in(stream_key, 1), dims, 0, int(grid[number_of - 1]))
    standing = jnp.searchsorted(jnp.asarray(grid, jnp.int32), pick, side="right")
    return jax.random.permutation(jax.random.fold_in(stream_key, 2), number_of)[standing].astype(jnp.int32)


def noise(own_key, shape, deviation, most, shards=(), kind=jnp.bfloat16):
    drawn = deviation * jax.random.normal(own_key, shape, jnp.float32)
    if shards:
        drawn = drawn * block_scale(own_key, shape, shards, -0.22, 0.18)
    return jnp.clip(drawn, -most, most).astype(kind)


def bell_draw_with(stream_key, extent, width, limit, cuts, heavy, kind=jnp.bfloat16):
    values = width * jax.random.normal(stream_key, extent, jnp.float32)
    if cuts:
        values = values * block_scale(stream_key, extent, cuts, -0.22, 0.18)
    return jnp.clip(raised(values, jax.random.fold_in(stream_key, 3), *heavy), -limit, limit).astype(kind)


def setup_inputs(seed: int = 0) -> dict:
    seeds = jax.random.split(jax.random.key(seed), 6)
    weights = noise(seeds[0], (2, N_GRP, 2, HR, E), 0.5, 4.0, ((0, 2), (1, 16)), jnp.float32)
    accum = jnp.clip(jnp.exp(math.log(1.0) - 4.6051702 * jax.random.uniform(seeds[1], (2, N_GRP, 2, HR), jnp.float32) ** block_scale(seeds[1], (2, N_GRP, 2, HR), ((0, 2), (1, 16)), -0.2, 0.2)), 0.01, 1.0)
    grads = bell_draw_with(seeds[2], (DEVICES, DEVICES, SLOTS, E), 1.0, 6.0, ((0, 32),), (0, 1, 32, 2.75), jnp.float32)
    row_ids = place_ends(ranked_ids(seeds[3], (DEVICES, DEVICES, SLOTS), 2 * HR, 2), jax.random.fold_in(seeds[3], 3), 0, (2 * HR) - 1).astype(jnp.int32)
    counts = draw_counts(jax.random.fold_in(seeds[5], 71), 0)
    return {"weights": weights, "accum": accum, "grads": grads, "row_ids": row_ids, "counts": counts}


LEARN_RATE = 0.5
EPSILON = 1e-06

def reference(weights, accum, grads, row_ids, counts):
    groups = N_GRP
    owners = 2 * groups
    moved = jnp.transpose(weights, (2, 1, 0, 3, 4)).reshape(owners, 2 * HR, E)
    moved_acc = jnp.transpose(accum, (2, 1, 0, 3)).reshape(owners, 2 * HR)
    slot_index = lax.broadcasted_iota(jnp.int32, (owners, owners, SLOTS), 2)
    live = slot_index < counts[:, :, None]
    masked = jnp.where(live[..., None], grads, jnp.zeros_like(grads))
    owner_index = lax.broadcasted_iota(jnp.int32, (owners, owners, SLOTS), 1)
    flat_rows = (owner_index * (2 * HR) + row_ids.astype(jnp.int32)).reshape(-1)
    total = jnp.zeros((owners * 2 * HR, E), jnp.float32).at[flat_rows].add(masked.reshape(-1, E))
    total = total.reshape(owners, 2 * HR, E)
    accumulated = moved_acc + lax.optimization_barrier(jnp.mean(total * total, axis=-1))
    updated = moved - LEARN_RATE * total / (jnp.sqrt(accumulated)[..., None] + EPSILON)
    return (updated.reshape(2, groups, 2, HR, E), accumulated.reshape(2, groups, 2, HR))
```

```python
import functools

import jax
import jax.numpy as jnp
from jax import lax
from jax.experimental import pallas as pl
from jax.experimental.pallas import tpu as pltpu
from jax.sharding import PartitionSpec as P

LEARN_RATE = 0.5
EPSILON = 1e-06
LANES = 128
MESH = pl.DeviceIdType.MESH
PIECES = 4


def exchange_kernel(
    halves, groups, weights, accum, grads, ids_t, counts,
    gotten, gotten_acc, got, got_ids,
    block_buf, id_pad, id_buf,
    local_sem, row_send, row_recv, acc_send, acc_recv, block_send, block_recv, id_send, id_recv,
):
    half = lax.axis_index("half")
    group = lax.axis_index("grp")
    owners = halves * groups
    me = half * groups + group
    other = 1 - half
    slots = ids_t.shape[0]
    piece = weights.shape[1] // PIECES

    def peer_of(step):
        peer = lax.rem(me + step, owners)
        return peer, (peer // groups, lax.rem(peer, groups))

    barrier = pltpu.get_barrier_semaphore()

    @pl.loop(1, owners)
    def _(step):
        _, where = peer_of(step)
        pl.semaphore_signal(barrier, inc=1, device_id=where, device_id_type=MESH)

    load = pltpu.make_async_copy(grads, block_buf, local_sem.at[0])
    load.start()
    slot = lax.broadcasted_iota(jnp.int32, ids_t.shape, 0)
    id_pad[...] = jnp.full(id_pad.shape, -1, jnp.int32)
    id_pad[0:slots, 0:owners] = jnp.where(slot < counts[...], ids_t[...], -1)
    turned = id_pad[...].T
    for owner in range(owners):
        id_buf[owner, 0:1, :] = turned[owner:owner + 1, :]
    load.wait()
    pl.semaphore_wait(barrier, owners - 1)

    def block_copy(step):
        peer, where = peer_of(step)
        return pltpu.make_async_remote_copy(
            src_ref=block_buf.at[peer], dst_ref=got.at[me],
            send_sem=block_send.at[peer], recv_sem=block_recv.at[me],
            device_id=where, device_id_type=MESH)

    def id_copy(step):
        peer, where = peer_of(step)
        return pltpu.make_async_remote_copy(
            src_ref=id_buf.at[peer], dst_ref=got_ids.at[me],
            send_sem=id_send.at[peer], recv_sem=id_recv.at[me],
            device_id=where, device_id_type=MESH)

    def row_copy(index):
        rows = pl.ds(index * piece, piece)
        return pltpu.make_async_remote_copy(
            src_ref=weights.at[other, rows], dst_ref=gotten.at[rows],
            send_sem=row_send.at[index], recv_sem=row_recv.at[index],
            device_id=(other, group), device_id_type=MESH)

    acc_copy = pltpu.make_async_remote_copy(
        src_ref=accum, dst_ref=gotten_acc, send_sem=acc_send, recv_sem=acc_recv,
        device_id=(other, group), device_id_type=MESH)

    @pl.loop(1, owners)
    def _(step):
        id_copy(step).start()
        block_copy(step).start()

    acc_copy.start()
    for index in range(PIECES):
        row_copy(index).start()
    own_block = pltpu.make_async_copy(block_buf.at[me], got.at[me], local_sem.at[0])
    own_ids = pltpu.make_async_copy(id_buf.at[me], got_ids.at[me], local_sem.at[1])
    own_block.start()
    own_ids.start()
    own_block.wait()
    own_ids.wait()

    @pl.loop(1, owners)
    def _(step):
        id_copy(step).wait_send()
        block_copy(step).wait_send()
        peer, where = peer_of(step)
        pltpu.make_async_remote_copy(
            src_ref=id_buf.at[peer], dst_ref=got_ids.at[peer],
            send_sem=id_send.at[peer], recv_sem=id_recv.at[peer],
            device_id=where, device_id_type=MESH).wait_recv()
        pltpu.make_async_remote_copy(
            src_ref=block_buf.at[peer], dst_ref=got.at[peer],
            send_sem=block_send.at[peer], recv_sem=block_recv.at[peer],
            device_id=where, device_id_type=MESH).wait_recv()

    acc_copy.wait()
    for index in range(PIECES):
        row_copy(index).wait()


def thirds(value):
    first = value.astype(jnp.bfloat16)
    rest = value - first.astype(jnp.float32)
    second = rest.astype(jnp.bfloat16)
    third = (rest - second.astype(jnp.float32)).astype(jnp.bfloat16)
    return jnp.concatenate([first, second, third], axis=1)


def joined(value, width):
    return value[:, 0:width] + value[:, width:2 * width] + value[:, 2 * width:3 * width]


def update_kernel(
    weights, accum, gotten, gotten_acc, got, got_ids, new_weights, new_accum,
    table, state, id_list, picked, delta, in_sem, out_sem, id_sem,
):
    half = lax.axis_index("half")
    senders, slots, width = got.shape
    count = senders * slots
    rows_half = weights.shape[1]
    piece = rows_half // PIECES
    spare = 2 * rows_half
    acc_rows = rows_half // LANES

    ids_in = pltpu.make_async_copy(got_ids, id_list, id_sem)
    ids_in.start()
    loads = []
    for index in range(PIECES):
        rows = pl.ds(index * piece, piece)
        kept_rows = pl.ds(pl.multiple_of(half * rows_half + index * piece, piece), piece)
        gotten_rows = pl.ds(pl.multiple_of((1 - half) * rows_half + index * piece, piece), piece)
        loads.append(pltpu.make_async_copy(
            weights.at[half, rows], table.at[kept_rows], in_sem.at[2 * index]))
        loads.append(pltpu.make_async_copy(
            gotten.at[rows], table.at[gotten_rows], in_sem.at[2 * index + 1]))
    for load in loads:
        load.start()
    table[spare:spare + 8, :] = jnp.zeros((8, width), jnp.float32)

    is_low = half == 0
    own = jnp.where(is_low, accum[0:1, :], accum[1:2, :])
    far = jnp.where(is_low, gotten_acc[0:1, :], gotten_acc[1:2, :])
    for old, line in enumerate((jnp.where(is_low, own, far), jnp.where(is_low, far, own))):
        for row in range(acc_rows):
            at = old * acc_rows + row
            state[at:at + 1, :] = line[:, row * LANES:(row + 1) * LANES]

    lane = lax.broadcasted_iota(jnp.int32, (count, LANES), 1)
    sub = lax.broadcasted_iota(jnp.int32, (count, LANES), 0)
    spread = jnp.broadcast_to(got_ids[...], (senders, slots, LANES)).reshape(count, LANES)
    mine = jnp.where(lane == lax.rem(sub, slots), spread, 0).astype(jnp.float32)
    column = jnp.sum(mine, axis=1, keepdims=True)
    wide = jnp.broadcast_to(column, (count, LANES))
    line = wide.T[0:1, :]
    grad_parts = thirds(got[...].reshape(count, width))
    old_state = state[...]
    state_parts = thirds(old_state)
    lane_f = lane.astype(jnp.float32)
    block = min(count, 512)
    gain = jnp.zeros((2 * acc_rows, 3 * LANES), jnp.float32)
    high_line = jnp.floor(line * (1.0 / LANES))
    for start in range(0, count, block):
        key = column[start:start + block]
        same = key == line
        hot = jnp.where(same, 1.0, 0.0)
        total = joined(jnp.dot(hot.astype(jnp.bfloat16), grad_parts,
                               preferred_element_type=jnp.float32), width)
        at_col = lax.broadcasted_iota(jnp.int32, (block, count), 1)
        at_row = lax.broadcasted_iota(jnp.int32, (block, count), 0) + start
        earlier = jnp.sum(jnp.where(at_col < at_row, hot, 0.0), axis=1, keepdims=True)
        high = jnp.floor(key * (1.0 / LANES))
        low = key - high * LANES
        row_hot = jnp.where(lane_f[:block] == high, 1.0, 0.0).astype(jnp.bfloat16) if acc_rows * 2 == LANES else jnp.where(
            lax.broadcasted_iota(jnp.int32, (block, 2 * acc_rows), 1).astype(jnp.float32) == high, 1.0, 0.0).astype(jnp.bfloat16)
        state_rows = joined(jnp.dot(row_hot, state_parts, preferred_element_type=jnp.float32), LANES)
        at_low = lane_f[:block] == low
        old_acc = jnp.sum(jnp.where(at_low, state_rows, 0.0), axis=1, keepdims=True)
        square = jnp.sum(total * total, axis=1, keepdims=True) * (1.0 / width)
        delta[start:start + block, :] = LEARN_RATE * total / (jnp.sqrt(old_acc + square) + EPSILON)
        once = jnp.where((earlier == 0.0) & (key >= 0.0), square, 0.0)
        add_parts = thirds(jnp.where(at_low, once, 0.0))
        high_of = high_line[:, start:start + block]
        tall = lax.broadcasted_iota(jnp.int32, (2 * acc_rows, block), 0).astype(jnp.float32)
        tall_hot = jnp.where(tall == high_of, 1.0, 0.0).astype(jnp.bfloat16)
        gain = gain + jnp.dot(tall_hot, add_parts, preferred_element_type=jnp.float32)
    state[...] = old_state + joined(gain, LANES)
    for old in range(2):
        for row in range(acc_rows):
            at = old * acc_rows + row
            new_accum[old:old + 1, row * LANES:(row + 1) * LANES] = state[at:at + 1, :]

    ids_in.wait()
    for load in loads:
        load.wait()

    def place(sender, slot):
        at = id_list[sender, 0, slot]
        return jnp.where(at < 0, spare, at)

    @pl.loop(0, senders)
    def _(sender):
        base = pl.multiple_of(sender * slots, slots)
        rows = [table[pl.ds(place(sender, slot), 1), :] for slot in range(slots)]
        for slot in range(slots):
            picked[pl.ds(base + slot, 1), :] = rows[slot]

    picked[...] = picked[...] - delta[...]

    @pl.loop(0, senders)
    def _(sender):
        base = pl.multiple_of(sender * slots, slots)
        rows = [picked[pl.ds(base + slot, 1), :] for slot in range(slots)]
        for slot in range(slots):
            table[pl.ds(place(sender, slot), 1), :] = rows[slot]

    stores = []
    for old in range(2):
        for index in range(PIECES):
            stores.append(pltpu.make_async_copy(
                table.at[pl.ds(old * rows_half + index * piece, piece)],
                new_weights.at[old, pl.ds(index * piece, piece)],
                out_sem.at[old * PIECES + index]))
    for store in stores:
        store.start()
    for store in stores:
        store.wait()


def per_device(halves, groups, weights, accum, grads, row_ids, counts):
    owners, slots, width = grads.shape[1:]
    rows_half = weights.shape[3]
    table = weights[0, 0]
    state = accum[0, 0]
    count = owners * slots
    any_space = pl.BlockSpec(memory_space=pl.ANY)
    vmem = pl.BlockSpec(memory_space=pltpu.VMEM)
    id_width = -(-owners // LANES) * LANES
    dma = pltpu.SemaphoreType.DMA
    gotten, gotten_acc, got, got_ids = pl.pallas_call(
        functools.partial(exchange_kernel, halves, groups),
        out_shape=(
            jax.ShapeDtypeStruct((rows_half, width), jnp.float32),
            jax.ShapeDtypeStruct((2, rows_half), jnp.float32),
            jax.ShapeDtypeStruct((owners, slots, width), jnp.float32),
            jax.ShapeDtypeStruct((owners, 1, LANES), jnp.int32),
        ),
        in_specs=[any_space, vmem, any_space, vmem, vmem],
        out_specs=(any_space, vmem, vmem, vmem),
        scratch_shapes=[
            pltpu.VMEM((owners, slots, width), jnp.float32),
            pltpu.VMEM((LANES, id_width), jnp.int32),
            pltpu.VMEM((owners, 1, LANES), jnp.int32),
            dma((2,)),
            dma((PIECES,)), dma((PIECES,)),
            dma, dma,
            dma((owners,)), dma((owners,)),
            dma((owners,)), dma((owners,)),
        ],
        compiler_params=pltpu.CompilerParams(collective_id=0, has_side_effects=True),
        name="exchange",
    )(table, state, grads[0], row_ids[0].T, counts)
    new_weights, new_accum = pl.pallas_call(
        update_kernel,
        out_shape=(
            jax.ShapeDtypeStruct((2, rows_half, width), jnp.float32),
            jax.ShapeDtypeStruct((2, rows_half), jnp.float32),
        ),
        in_specs=[any_space, vmem, any_space, vmem, vmem, vmem],
        out_specs=(any_space, vmem),
        scratch_shapes=[
            pltpu.VMEM((2 * rows_half + 8, width), jnp.float32),
            pltpu.VMEM((2 * rows_half // LANES, LANES), jnp.float32),
            pltpu.SMEM((owners, 1, LANES), jnp.int32),
            pltpu.VMEM((count, width), jnp.float32),
            pltpu.VMEM((count, width), jnp.float32),
            dma((2 * PIECES,)), dma((2 * PIECES,)), dma,
        ],
        name="update",
    )(table, state, gotten, gotten_acc, got, got_ids)
    return new_weights[None, None], new_accum[None, None]


def solution(mesh):
    placed = (
        P("half", "grp", None, None, None),
        P("half", "grp", None, None),
        P(("half", "grp"), None, None, None),
        P(("half", "grp"), None, None),
        P(("half", "grp"), None),
    )
    return jax.shard_map(
        functools.partial(per_device, mesh.shape["half"], mesh.shape["grp"]),
        mesh=mesh,
        in_specs=placed,
        out_specs=(P("half", "grp", None, None, None), P("half", "grp", None, None)),
        check_vma=False,
    )
```

```python
import functools

import jax
import jax.numpy as jnp
from jax import lax
from jax.experimental import pallas as pl
from jax.experimental.pallas import tpu as pltpu
from jax.sharding import PartitionSpec as P

LEARN_RATE = 0.5
EPSILON = 1e-06
LANES = 128
MESH = pl.DeviceIdType.MESH
PIECES = 4


def exchange_kernel(
    halves, groups, weights, accum, grads, ids_t, counts,
    table, pair_acc, got, got_ids,
    block_buf, id_in, count_in, id_pad, id_buf,
    local_sem, row_send, row_recv, acc_send, acc_recv, block_send, block_recv, id_send, id_recv,
):
    half = lax.axis_index("half")
    group = lax.axis_index("grp")
    owners = halves * groups
    me = half * groups + group
    other = 1 - half
    slots = ids_t.shape[0]
    rows_half = weights.shape[1]
    piece = rows_half // PIECES
    home = pl.multiple_of(half * rows_half, rows_half)

    def peer_of(step):
        peer = lax.rem(me + step, owners)
        return peer, (peer // groups, lax.rem(peer, groups))

    barrier = pltpu.get_barrier_semaphore()

    @pl.loop(1, owners)
    def _(step):
        _, where = peer_of(step)
        pl.semaphore_signal(barrier, inc=1, device_id=where, device_id_type=MESH)

    id_load = pltpu.make_async_copy(ids_t, id_in, local_sem.at[1])
    count_load = pltpu.make_async_copy(counts, count_in, local_sem.at[2])
    load = pltpu.make_async_copy(grads, block_buf, local_sem.at[0])
    keep = pltpu.make_async_copy(
        weights.at[half], table.at[pl.ds(home, rows_half)], local_sem.at[3])
    keep_acc = pltpu.make_async_copy(accum, pair_acc.at[half], local_sem.at[4])
    id_load.start()
    count_load.start()
    keep_acc.start()
    load.start()
    keep.start()
    id_load.wait()
    count_load.wait()
    slot = lax.broadcasted_iota(jnp.int32, ids_t.shape, 0)
    id_pad[...] = jnp.full(id_pad.shape, -1, jnp.int32)
    id_pad[0:slots, 0:owners] = jnp.where(slot < count_in[...], id_in[...], -1)
    turned = id_pad[...].T
    for owner in range(owners):
        id_buf[owner, 0:1, :] = turned[owner:owner + 1, :]
    load.wait()
    pl.semaphore_wait(barrier, owners - 1)

    def block_copy(step):
        peer, where = peer_of(step)
        return pltpu.make_async_remote_copy(
            src_ref=block_buf.at[peer], dst_ref=got.at[me],
            send_sem=block_send.at[peer], recv_sem=block_recv.at[me],
            device_id=where, device_id_type=MESH)

    def id_copy(step):
        peer, where = peer_of(step)
        return pltpu.make_async_remote_copy(
            src_ref=id_buf.at[peer], dst_ref=got_ids.at[me],
            send_sem=id_send.at[peer], recv_sem=id_recv.at[me],
            device_id=where, device_id_type=MESH)

    def row_copy(index):
        rows = pl.ds(index * piece, piece)
        return pltpu.make_async_remote_copy(
            src_ref=weights.at[other, rows],
            dst_ref=table.at[pl.ds(pl.multiple_of(home + index * piece, piece), piece)],
            send_sem=row_send.at[index], recv_sem=row_recv.at[index],
            device_id=(other, group), device_id_type=MESH)

    acc_copy = pltpu.make_async_remote_copy(
        src_ref=accum, dst_ref=pair_acc.at[half], send_sem=acc_send, recv_sem=acc_recv,
        device_id=(other, group), device_id_type=MESH)

    @pl.loop(1, owners)
    def _(step):
        id_copy(step).start()
        block_copy(step).start()

    acc_copy.start()
    for index in range(PIECES):
        row_copy(index).start()
    own_block = pltpu.make_async_copy(block_buf.at[me], got.at[me], local_sem.at[0])
    own_ids = pltpu.make_async_copy(id_buf.at[me], got_ids.at[me], local_sem.at[1])
    own_block.start()
    own_ids.start()
    own_block.wait()
    own_ids.wait()
    keep.wait()
    keep_acc.wait()

    @pl.loop(1, owners)
    def _(step):
        id_copy(step).wait_send()
        block_copy(step).wait_send()
        peer, where = peer_of(step)
        pltpu.make_async_remote_copy(
            src_ref=id_buf.at[peer], dst_ref=got_ids.at[peer],
            send_sem=id_send.at[peer], recv_sem=id_recv.at[peer],
            device_id=where, device_id_type=MESH).wait_recv()
        pltpu.make_async_remote_copy(
            src_ref=block_buf.at[peer], dst_ref=got.at[peer],
            send_sem=block_send.at[peer], recv_sem=block_recv.at[peer],
            device_id=where, device_id_type=MESH).wait_recv()

    acc_copy.wait()
    for index in range(PIECES):
        row_copy(index).wait()


def thirds(value):
    first = value.astype(jnp.bfloat16)
    rest = value - first.astype(jnp.float32)
    second = rest.astype(jnp.bfloat16)
    third = (rest - second.astype(jnp.float32)).astype(jnp.bfloat16)
    return jnp.concatenate([first, second, third], axis=1)


def joined(value, width):
    return value[:, 0:width] + value[:, width:2 * width] + value[:, 2 * width:3 * width]


def update_kernel(
    table_in, pair_acc, got, got_ids, table, new_weights, new_accum,
    out_acc, state, id_list, picked, delta, in_sem, out_sem, id_sem,
):
    half = lax.axis_index("half")
    senders, slots, width = got.shape
    count = senders * slots
    rows_half = pair_acc.shape[2]
    piece = rows_half // PIECES
    spare = 2 * rows_half
    acc_rows = rows_half // LANES

    ids_in = pltpu.make_async_copy(got_ids, id_list, id_sem)
    ids_in.start()
    table[spare:spare + 8, :] = jnp.zeros((8, width), jnp.float32)

    is_low = half == 0
    for old in range(2):
        line = jnp.where(is_low, pair_acc[old, 0:1, :], pair_acc[old, 1:2, :])
        for row in range(acc_rows):
            at = old * acc_rows + row
            state[at:at + 1, :] = line[:, row * LANES:(row + 1) * LANES]

    lane = lax.broadcasted_iota(jnp.int32, (count, LANES), 1)
    sub = lax.broadcasted_iota(jnp.int32, (count, LANES), 0)
    spread = jnp.broadcast_to(got_ids[...], (senders, slots, LANES)).reshape(count, LANES)
    mine = jnp.where(lane == lax.rem(sub, slots), spread, 0).astype(jnp.float32)
    column = jnp.sum(mine, axis=1, keepdims=True)
    wide = jnp.broadcast_to(column, (count, LANES))
    line = wide.T[0:1, :]
    grad_parts = thirds(got[...].reshape(count, width))
    old_state = state[...]
    state_parts = thirds(old_state)
    lane_f = lane.astype(jnp.float32)
    block = min(count, 512)
    gain = jnp.zeros((2 * acc_rows, 3 * LANES), jnp.float32)
    high_line = jnp.floor(line * (1.0 / LANES))
    for start in range(0, count, block):
        key = column[start:start + block]
        same = key == line
        hot = jnp.where(same, 1.0, 0.0)
        total = joined(jnp.dot(hot.astype(jnp.bfloat16), grad_parts,
                               preferred_element_type=jnp.float32), width)
        at_col = lax.broadcasted_iota(jnp.int32, (block, count), 1)
        at_row = lax.broadcasted_iota(jnp.int32, (block, count), 0) + start
        earlier = jnp.sum(jnp.where(at_col < at_row, hot, 0.0), axis=1, keepdims=True)
        high = jnp.floor(key * (1.0 / LANES))
        low = key - high * LANES
        row_hot = jnp.where(lane_f[:block] == high, 1.0, 0.0).astype(jnp.bfloat16) if acc_rows * 2 == LANES else jnp.where(
            lax.broadcasted_iota(jnp.int32, (block, 2 * acc_rows), 1).astype(jnp.float32) == high, 1.0, 0.0).astype(jnp.bfloat16)
        state_rows = joined(jnp.dot(row_hot, state_parts, preferred_element_type=jnp.float32), LANES)
        at_low = lane_f[:block] == low
        old_acc = jnp.sum(jnp.where(at_low, state_rows, 0.0), axis=1, keepdims=True)
        square = jnp.sum(total * total, axis=1, keepdims=True) * (1.0 / width)
        delta[start:start + block, :] = LEARN_RATE * total / (jnp.sqrt(old_acc + square) + EPSILON)
        once = jnp.where((earlier == 0.0) & (key >= 0.0), square, 0.0)
        add_parts = thirds(jnp.where(at_low, once, 0.0))
        high_of = high_line[:, start:start + block]
        tall = lax.broadcasted_iota(jnp.int32, (2 * acc_rows, block), 0).astype(jnp.float32)
        tall_hot = jnp.where(tall == high_of, 1.0, 0.0).astype(jnp.bfloat16)
        gain = gain + jnp.dot(tall_hot, add_parts, preferred_element_type=jnp.float32)
    state[...] = old_state + joined(gain, LANES)
    for old in range(2):
        for row in range(acc_rows):
            at = old * acc_rows + row
            out_acc[old:old + 1, row * LANES:(row + 1) * LANES] = state[at:at + 1, :]

    acc_out = pltpu.make_async_copy(out_acc, new_accum, in_sem)
    acc_out.start()
    ids_in.wait()

    def place(sender, slot):
        at = id_list[sender, 0, slot]
        return jnp.where(at < 0, spare, at)

    @pl.loop(0, senders)
    def _(sender):
        base = pl.multiple_of(sender * slots, slots)
        rows = [table[pl.ds(place(sender, slot), 1), :] for slot in range(slots)]
        for slot in range(slots):
            picked[pl.ds(base + slot, 1), :] = rows[slot]

    picked[...] = picked[...] - delta[...]

    @pl.loop(0, senders)
    def _(sender):
        base = pl.multiple_of(sender * slots, slots)
        rows = [picked[pl.ds(base + slot, 1), :] for slot in range(slots)]
        for slot in range(slots):
            table[pl.ds(place(sender, slot), 1), :] = rows[slot]

    stores = []
    for old in range(2):
        for index in range(PIECES):
            stores.append(pltpu.make_async_copy(
                table.at[pl.ds(old * rows_half + index * piece, piece)],
                new_weights.at[old, pl.ds(index * piece, piece)],
                out_sem.at[old * PIECES + index]))
    for store in stores:
        store.start()
    for store in stores:
        store.wait()
    acc_out.wait()


def per_device(halves, groups, weights, accum, grads, row_ids, counts):
    owners, slots, width = grads.shape[1:]
    rows_half = weights.shape[3]
    table = weights[0, 0]
    state = accum[0, 0]
    count = owners * slots
    hbm = pl.BlockSpec(memory_space=pltpu.HBM)
    vmem = pl.BlockSpec(memory_space=pltpu.VMEM)
    id_width = -(-owners // LANES) * LANES
    dma = pltpu.SemaphoreType.DMA
    landed = (
        jax.ShapeDtypeStruct((2 * rows_half + 8, width), jnp.float32),
        jax.ShapeDtypeStruct((2, 2, rows_half), jnp.float32),
        jax.ShapeDtypeStruct((owners, slots, width), jnp.float32),
        jax.ShapeDtypeStruct((owners, 1, LANES), jnp.int32),
    )
    moved, pair_acc, got, got_ids = pl.pallas_call(
        functools.partial(exchange_kernel, halves, groups),
        out_shape=landed,
        in_specs=[hbm] * 5,
        out_specs=(vmem,) * 4,
        scratch_shapes=[
            pltpu.VMEM((owners, slots, width), jnp.float32),
            pltpu.VMEM((slots, owners), jnp.int32),
            pltpu.VMEM((1, owners), jnp.int32),
            pltpu.VMEM((LANES, id_width), jnp.int32),
            pltpu.VMEM((owners, 1, LANES), jnp.int32),
            dma((5,)),
            dma((PIECES,)), dma((PIECES,)),
            dma, dma,
            dma((owners,)), dma((owners,)),
            dma((owners,)), dma((owners,)),
        ],
        compiler_params=pltpu.CompilerParams(
            collective_id=0, has_side_effects=True, vmem_limit_bytes=16 << 20),
        name="exchange",
    )(*(pltpu.with_memory_space_constraint(value, pltpu.HBM)
        for value in (table, state, grads[0], row_ids[0].T, counts)))
    _, new_weights, new_accum = pl.pallas_call(
        update_kernel,
        out_shape=(
            jax.ShapeDtypeStruct((2 * rows_half + 8, width), jnp.float32),
            jax.ShapeDtypeStruct((2, rows_half, width), jnp.float32),
            jax.ShapeDtypeStruct((2, rows_half), jnp.float32),
        ),
        in_specs=[vmem] * 4,
        out_specs=(vmem, hbm, hbm),
        scratch_shapes=[
            pltpu.VMEM((2, rows_half), jnp.float32),
            pltpu.VMEM((2 * rows_half // LANES, LANES), jnp.float32),
            pltpu.SMEM((owners, 1, LANES), jnp.int32),
            pltpu.VMEM((count, width), jnp.float32),
            pltpu.VMEM((count, width), jnp.float32),
            dma, dma((2 * PIECES,)), dma,
        ],
        input_output_aliases={0: 0},
        compiler_params=pltpu.CompilerParams(vmem_limit_bytes=32 << 20),
        name="update",
    )(moved, pair_acc, got, got_ids)
    return new_weights[None, None], new_accum[None, None]


def solution(mesh):
    placed = (
        P("half", "grp", None, None, None),
        P("half", "grp", None, None),
        P(("half", "grp"), None, None, None),
        P(("half", "grp"), None, None),
        P(("half", "grp"), None),
    )
    return jax.shard_map(
        functools.partial(per_device, mesh.shape["half"], mesh.shape["grp"]),
        mesh=mesh,
        in_specs=placed,
        out_specs=(P("half", "grp", None, None, None), P("half", "grp", None, None)),
        check_vma=False,
    )
```
